32 devices in a mesh: row: 2 (over x), col: 4 (over y, core), layer: 4 (over z).
Axes of the slice: x: 2, y: 2, z: 4, core: 2. Of those that a mesh axis runs over, the one named last changes fastest.
Arguments:
- a_cyclic: float32 [4, 1024, 4096], P('layer', 'row', 'col'), may hold values from -6 to 6
- a_mask: int32 [4, 8, 32], P('layer', 'row', 'col'), may hold values from 0 to 1, as said below
- b_dense: float32 [16384, 16384], P('row', ('col', 'layer')), may hold values from -0.21875 to 0.21875
- b_mask: int32 [128, 128], P('row', ('col', 'layer')), may hold values from 0 to 1, as said below
Outputs:
- product: float32 [1024, 16384], P('row', ('col', 'layer'))
The draws below stay inside these ranges and needn't reach their ends.
Inputs may be any that keep to these rules, and one draw needn't show every extreme that they name: For each l, each run of 4 block rows starting at a multiple of 4 and each run of 8 block columns starting at a multiple of 8, those blocks of a_mask[l] hold 1 to 12 ones. In every draw, for some l and some row run, the groups of all 4 column runs hold exactly 12. `b_mask`: take the block rows r * 64 to (r + 1) * 64 - 1, a residue d modulo 4, and the block columns g * 8 to (g + 1) * 8 - 1: the blocks among them whose row index is d modulo 4 hold 1 to 48 ones. In every draw, for some r, d and c, the groups of all g from c * 4 to c * 4 + 3 hold exactly 48.
All inputs are finite; a program needn't handle non-finite values.
Results may differ from the reference program's by a relative error of at most 0.00007.
Values sent between devices are 32-bit elements; how exact they have to be, the bound alone decides.
A program may use at most 256 MiB of HBM per device.

```python
import jax
import jax.numpy as jnp
from jax import lax

BS = 128
K = 16384
N = 16384
MBR = 4
M = 1024
KB = 128
NB = 128
KBL = 32
KRB = 64
JCB = 8
QC = 8
XCAP = 48
ACAP = 12
N_ROW = 2
N_COL = 4
N_LAYER = 4


def draw_a_mask(key, part):
    members = MBR * QC
    groups = N_LAYER * N_ROW * N_COL
    count_key = jax.random.fold_in(key, 11)
    order_key = jax.random.fold_in(key, 12)
    layer_key = jax.random.fold_in(key, 13)
    row_key = jax.random.fold_in(key, 14)
    counts = jax.random.randint(count_key, (N_LAYER, N_ROW, N_COL), 1, ACAP + 1)
    layer_pick = jax.random.randint(layer_key, (), 0, N_LAYER)
    row_pick = jax.random.randint(row_key, (), 0, N_ROW)
    layer_ids = jnp.arange(N_LAYER)[:, None, None]
    row_ids = jnp.arange(N_ROW)[None, :, None]
    counts = jnp.where((layer_ids == layer_pick) & (row_ids == row_pick), ACAP, counts)

    def shuffle(group_key):
        return jax.random.permutation(group_key, members)
    orders = jax.vmap(shuffle)(jax.random.split(order_key, groups))
    occupied = (orders.reshape(N_LAYER, N_ROW, N_COL, members) < counts[..., None]).astype(jnp.int32)
    shaped = occupied.reshape(N_LAYER, N_ROW, N_COL, MBR, QC).transpose(0, 1, 3, 2, 4)
    return shaped.reshape(N_LAYER, N_ROW * MBR, N_COL * QC)


def draw_b_mask(key, part):
    per_layer = KRB // N_LAYER
    members = per_layer * JCB
    runs = N_COL * N_LAYER
    groups = N_ROW * N_LAYER * runs
    count_key = jax.random.fold_in(key, 21)
    order_key = jax.random.fold_in(key, 22)
    row_key = jax.random.fold_in(key, 23)
    residue_key = jax.random.fold_in(key, 24)
    col_key = jax.random.fold_in(key, 25)
    counts = jax.random.randint(count_key, (N_ROW, N_LAYER, runs), 1, XCAP + 1)
    row_pick = jax.random.randint(row_key, (), 0, N_ROW)
    residue_pick = jax.random.randint(residue_key, (), 0, N_LAYER)
    col_pick = jax.random.randint(col_key, (), 0, N_COL)
    row_ids = jnp.arange(N_ROW)[:, None, None]
    residue_ids = jnp.arange(N_LAYER)[None, :, None]
    run_ids = jnp.arange(runs)[None, None, :]
    forced = (row_ids == row_pick) & (residue_ids == residue_pick) & (run_ids // N_LAYER == col_pick)
    counts = jnp.where(forced, XCAP, counts)

    def shuffle(group_key):
        return jax.random.permutation(group_key, members)
    orders = jax.vmap(shuffle)(jax.random.split(order_key, groups))
    occupied = (orders.reshape(N_ROW, N_LAYER, runs, members) < counts[..., None]).astype(jnp.int32)
    shaped = occupied.reshape(N_ROW, N_LAYER, runs, per_layer, JCB).transpose(0, 3, 1, 2, 4)
    return shaped.reshape(KB, NB)


def steps_of(rng, dims, shards, least, top_value):
    factor_of = 1.0
    for dim, shards_of in shards:
        heights = jax.random.uniform(jax.random.fold_in(jax.random.fold_in(rng, 6), dim), (shards_of,), jnp.float32, least / len(shards), top_value / len(shards))
        factor_of = factor_of * jnp.repeat(jnp.exp(heights), dims[dim] // shards_of).reshape((-1,) + (1,) * (len(dims) - 1 - dim))
    return factor_of


def normal_values(stream_key, extent, deviation, bound, shards=(), dtype=jnp.bfloat16):
    factor_of = steps_of(stream_key, extent, shards, -0.22, 0.18) if shards else 1.0
    values = jax.random.normal(stream_key, extent, jnp.float32) * deviation * factor_of
    return jnp.minimum(jnp.maximum(values, -bound), bound).astype(dtype)


def setup_inputs(seed: int = 0) -> dict:
    seeds = jax.random.split(jax.random.key(seed), 5)
    return {
        "a_cyclic": normal_values(seeds[0], (N_LAYER, M, KBL * BS), 1.0, 6.0, ((0, 4), (1, 2), (2, 4)), jnp.float32),
        "a_mask": draw_a_mask(jax.random.fold_in(seeds[4], 71), 0),
        "b_dense": normal_values(seeds[2], (K, N), (K // 20) ** -0.5, 0.21875, ((0, 2), (1, 16)), jnp.float32),
        "b_mask": draw_b_mask(jax.random.fold_in(seeds[4], 71), 0),
    }


def reference(a_cyclic, a_mask, b_dense, b_mask):
    layers, row_count, columns = a_cyclic.shape
    q_count = columns // BS
    a_scale = jnp.repeat(jnp.repeat(a_mask.astype(jnp.float32), BS, axis=1), BS, axis=2)
    masked = a_cyclic * a_scale
    a_full = masked.reshape(layers, row_count, q_count, BS).transpose(1, 2, 0, 3).reshape(row_count, layers * columns)
    b_scale = jnp.repeat(jnp.repeat(b_mask.astype(jnp.float32), BS, axis=0), BS, axis=1)
    b_full = b_dense * b_scale
    return jnp.dot(a_full, b_full, preferred_element_type=jnp.float32, precision=lax.Precision.HIGHEST)
```

```python
import functools

import jax
import jax.numpy as jnp
from jax import lax
from jax.experimental import pallas as pl
from jax.experimental.pallas import tpu as pltpu
from jax.sharding import PartitionSpec as P

precise = lax.Precision.HIGHEST


def to_blocks(matrix, block_size):
    row_blocks = matrix.shape[0] // block_size
    col_blocks = matrix.shape[1] // block_size
    shaped = matrix.reshape(row_blocks, block_size, col_blocks, block_size).transpose(0, 2, 1, 3)
    return shaped.reshape(row_blocks * col_blocks, block_size, block_size)


def pack_blocks(blocks, is_live, capacity):
    total_places = is_live.shape[0]
    rank_of = jnp.cumsum(is_live) - 1
    slot_numbers = jnp.arange(capacity, dtype=jnp.int32)
    chosen = (is_live[None, :] > 0) & (rank_of[None, :] == slot_numbers[:, None])
    weights = chosen.astype(jnp.float32)
    packed = jnp.einsum("cg,gxy->cxy", weights, blocks, precision=precise)
    places = jnp.arange(total_places, dtype=jnp.int32)
    any_match = jnp.any(chosen, axis=1)
    position = jnp.sum(jnp.where(chosen, places[None, :], 0), axis=1)
    slot_ids = jnp.where(any_match, position, -1)
    return (packed, slot_ids)


def lookup_table(gathered, key_of, key_count):
    slot_count = gathered.shape[0]
    key_values = jnp.arange(key_count, dtype=jnp.int32)
    matches = key_of[:, None] == key_values[None, :]
    any_match = jnp.any(matches, axis=0)
    slot_numbers = jnp.arange(slot_count, dtype=jnp.int32)
    slot_index = jnp.sum(jnp.where(matches, slot_numbers[:, None], 0), axis=0)
    slot_of = jnp.where(any_match, slot_index, slot_count)
    padded = jnp.concatenate([gathered, jnp.zeros((1,) + gathered.shape[1:], jnp.float32)], axis=0)
    return (padded, slot_of)


def accumulate(running, slot_data, slot_ids, source, padded, slot_of, k_step, jwidth):
    row_blocks = running.shape[0]
    is_live = slot_ids >= 0
    clipped = jnp.maximum(slot_ids, 0)
    k_index = source * k_step + clipped // jwidth
    column = clipped % jwidth
    rows_here = jnp.arange(row_blocks, dtype=jnp.int32)
    where_rows = slot_of[k_index[:, None] * row_blocks + rows_here[None, :]]
    a_pieces = padded[where_rows]
    b_pieces = jnp.where(is_live[:, None, None], slot_data, 0.0)
    products = jnp.einsum("smxa,sab->smxb", a_pieces, b_pieces, precision=precise)
    spread = (
        (column[:, None] == jnp.arange(jwidth, dtype=jnp.int32)[None, :]) & is_live[:, None]
    ).astype(jnp.float32)
    return running + jnp.einsum("smxb,sj->mxjb", products, spread, precision=precise)


def make_folder(padded, slot_of, k_step, jwidth, shard):

    def fold_piece(running, portion, offset):
        slot_data, slot_ids = portion
        sources = slot_data.shape[0] // shard
        slot_groups = slot_data.reshape((sources, shard) + slot_data.shape[1:])
        id_groups = slot_ids.reshape(sources, shard)
        source_rows = jnp.arange(sources, dtype=jnp.int32)

        def add_source(carry, inputs):
            group_slots, group_ids, source = inputs
            return (
                accumulate(carry, group_slots, group_ids, source, padded, slot_of, k_step, jwidth),
                None,
            )

        result, unused = lax.scan(add_source, running, (slot_groups, id_groups, source_rows))
        return result

    return fold_piece


def on_device(a_cyclic, a_mask, b_dense, b_mask):
    block_size = a_cyclic.shape[1] // a_mask.shape[1]
    layer_count = lax.axis_size("layer")
    row_count = lax.axis_size("row")
    row_blocks = a_mask.shape[1]
    q_blocks = a_mask.shape[2]
    k_run = b_mask.shape[0]
    j_run = b_mask.shape[1]
    per_layer = k_run // layer_count
    a_capacity = max(2, row_blocks * q_blocks * 3 // 8)
    b_capacity = max(2, per_layer * j_run * 3 // 8)
    a_blocks = to_blocks(a_cyclic[0], block_size)
    a_slots, a_ids = pack_blocks(a_blocks, a_mask[0].reshape(-1), a_capacity)
    b_blocks = to_blocks(b_dense, block_size)
    gathered, gathered_ids = (
        lax.all_gather(a_slots, ("col", "layer"), axis=0, tiled=True),
        lax.all_gather(a_ids, ("col", "layer"), axis=0, tiled=True),
    )
    from_device = jnp.arange(gathered.shape[0], dtype=jnp.int32) // a_capacity
    from_col = from_device // layer_count
    from_layer = from_device % layer_count
    clipped = jnp.maximum(gathered_ids, 0)
    k_index = (from_col * q_blocks + clipped % q_blocks) * layer_count + from_layer
    key_of = jnp.where(gathered_ids >= 0, k_index * row_blocks + clipped // q_blocks, -1)
    padded, slot_of = lookup_table(gathered, key_of, k_run * row_count * row_blocks)
    b_slots, b_ids = pack_blocks(b_blocks, b_mask.reshape(-1), layer_count * b_capacity)
    zero_sum = jnp.zeros((row_blocks, block_size, j_run, block_size), jnp.float32)
    folder = make_folder(padded, slot_of, k_run, j_run, layer_count * b_capacity)
    running = folder(
        zero_sum,
        (
            lax.all_gather(b_slots, "row", axis=0, tiled=True),
            lax.all_gather(b_ids, "row", axis=0, tiled=True),
        ),
        jnp.int32(0),
    )
    return running.reshape(row_blocks * block_size, j_run * block_size)


CHUNK = 2
DEPTH = 4
MASK_ROWS = 8


def pack_kernel(block_size, capacity, places, mask_ref, a_ref, out_ref, sems):
    copies = []
    for slot in range(capacity):
        row = pl.multiple_of(places[0, slot] * block_size, block_size)
        column = pl.multiple_of(places[1, slot] * block_size, block_size)
        copies.append(
            pltpu.make_async_copy(
                a_ref.at[pl.ds(row, block_size), pl.ds(column, block_size)],
                out_ref.at[pl.ds(slot * block_size, block_size), :],
                sems.at[slot],
            )
        )
    for copy in copies:
        copy.start()
    out_ref[pl.ds(capacity * block_size, MASK_ROWS), :] = mask_ref[...]
    for copy in copies:
        copy.wait()


def pack_a(a_local, mask, block_size, capacity):
    row_blocks, q_blocks = mask.shape
    flat = mask.reshape(-1)
    spots = row_blocks * q_blocks
    order = jnp.arange(spots, dtype=jnp.int32)
    before = jnp.sum(jnp.where(order[None, :] < order[:, None], flat[None, :], 0), axis=1)
    slots = jnp.arange(capacity, dtype=jnp.int32)
    chosen = (flat[None, :] > 0) & (before[None, :] == slots[:, None])
    position = jnp.sum(jnp.where(chosen, order[None, :], 0), axis=1)
    places = jnp.stack([position // q_blocks, position % q_blocks])
    mask_rows = jnp.zeros((MASK_ROWS, block_size), jnp.float32)
    mask_rows = mask_rows.at[0, :spots].set(flat.astype(jnp.float32))
    return pl.pallas_call(
        functools.partial(pack_kernel, block_size, capacity),
        out_shape=jax.ShapeDtypeStruct((capacity * block_size + MASK_ROWS, block_size), jnp.float32),
        in_specs=[
            pl.BlockSpec(memory_space=pltpu.SMEM),
            pl.BlockSpec(memory_space=pltpu.VMEM),
            pl.BlockSpec(memory_space=pl.ANY),
        ],
        out_specs=pl.BlockSpec(memory_space=pltpu.VMEM),
        scratch_shapes=[pltpu.SemaphoreType.DMA((capacity,))],
    )(places, mask_rows, a_local)


def split(value):
    high = value.astype(jnp.bfloat16)
    low = (value - high.astype(jnp.float32)).astype(jnp.bfloat16)
    return high, low


def product_kernel(
    block_size, all_rows, k_run, table, scale_ref, a_ref, b_ref, theirs_ref, mine_ref,
    total, tile, high_ref, low_ref, offset_of, row_of, sems
):
    def fetch(k):
        slot = lax.rem(k, DEPTH)
        row = pl.multiple_of(k * block_size, block_size)
        return pltpu.make_async_copy(
            b_ref.at[pl.ds(row, block_size), :], tile.at[slot], sems.at[slot]
        )

    for k in range(DEPTH - 1):
        fetch(k).start()
    total[...] = jnp.zeros_like(total)

    @pl.loop(0, k_run)
    def step(k):
        @pl.when(k + DEPTH - 1 < k_run)
        def ahead():
            fetch(k + DEPTH - 1).start()

        count = jnp.int32(0)
        for m in range(all_rows):
            offset = table[k * all_rows + m]
            offset_of[count] = offset
            row_of[count] = m
            count = count + (offset >= 0).astype(jnp.int32)
        for extra in range(CHUNK - 1):
            offset_of[count + extra] = 0
            row_of[count + extra] = all_rows
        fetch(k).wait()

        @pl.when(count > 0)
        def used():
            slot = lax.rem(k, DEPTH)
            high, low = split(tile[slot] * scale_ref[pl.ds(k, 1), :])
            high_ref[pl.ds(0, block_size), :] = high
            high_ref[pl.ds(block_size, block_size), :] = high
            low_ref[pl.ds(0, block_size), :] = low
            low_ref[pl.ds(block_size, block_size), :] = low

            @pl.loop(0, (count + CHUNK - 1) // CHUNK)
            def chunk(c):
                pieces = []
                for i in range(CHUNK):
                    start = pl.multiple_of(offset_of[c * CHUNK + i], MASK_ROWS)
                    a_high, a_low = split(a_ref[pl.ds(start, block_size), :])
                    pieces.append(jnp.concatenate([a_high, a_low], axis=1))
                left = jnp.concatenate(pieces, axis=0)
                part = jnp.dot(left, high_ref[...], preferred_element_type=jnp.float32)
                part = part + jnp.dot(left, low_ref[...], preferred_element_type=jnp.float32)
                for i in range(CHUNK):
                    row = pl.multiple_of(row_of[c * CHUNK + i] * block_size, block_size)
                    total[pl.ds(row, block_size), :] += part[i * block_size:(i + 1) * block_size]

    half = theirs_ref.shape[0]
    theirs_ref[...] = total[pl.ds(0, half), :]
    mine_ref[...] = total[pl.ds(half, half), :]


def multiply(table, scale, gathered, b_local, block_size, all_rows):
    k_size, width = b_local.shape
    k_run = k_size // block_size
    half = all_rows // 2 * block_size
    result = jax.ShapeDtypeStruct((half, width), jnp.float32)
    vmem = pl.BlockSpec(memory_space=pltpu.VMEM)
    return pl.pallas_call(
        functools.partial(product_kernel, block_size, all_rows, k_run),
        out_shape=(result, result),
        in_specs=[
            pl.BlockSpec(memory_space=pltpu.SMEM),
            vmem,
            vmem,
            pl.BlockSpec(memory_space=pl.ANY),
        ],
        out_specs=(vmem, vmem),
        scratch_shapes=[
            pltpu.VMEM(((all_rows + 1) * block_size, width), jnp.float32),
            pltpu.VMEM((DEPTH, block_size, width), jnp.float32),
            pltpu.VMEM((2 * block_size, width), jnp.bfloat16),
            pltpu.VMEM((2 * block_size, width), jnp.bfloat16),
            pltpu.SMEM((all_rows + CHUNK,), jnp.int32),
            pltpu.SMEM((all_rows + CHUNK,), jnp.int32),
            pltpu.SemaphoreType.DMA((DEPTH,)),
        ],
        compiler_params=pltpu.CompilerParams(vmem_limit_bytes=60 * 1024 * 1024),
    )(table, scale, gathered, b_local)


def gather_a(payload, cols_per_row):
    row_count, col_count = lax.axis_size("row"), lax.axis_size("col")
    pairs = []
    for row in range(row_count):
        for col in range(col_count):
            target = (col // cols_per_row) * col_count + row * cols_per_row + col % cols_per_row
            pairs.append((row * col_count + col, target))
    moved = lax.ppermute(payload, ("row", "col"), pairs)
    return lax.all_gather(moved, ("col", "layer"), axis=0, tiled=True)


def on_pair_device(a_cyclic, a_mask, b_dense, b_mask):
    row_blocks, q_blocks = a_mask.shape[1:]
    block_size = a_cyclic.shape[1] // row_blocks
    layer_count, row_count = lax.axis_size("layer"), lax.axis_size("row")
    cols_per_row = lax.axis_size("col") // row_count
    capacity = max(2, row_blocks * q_blocks * 3 // 8)
    all_rows = row_blocks * row_count
    payload = pack_a(a_cyclic[0], a_mask[0], block_size, capacity)
    gathered = gather_a(payload, cols_per_row)
    spots = row_blocks * q_blocks
    stride = payload.shape[0]
    sources = gathered.shape[0] // stride
    mask = gathered.reshape(sources, stride, block_size)[:, capacity * block_size, :spots]
    order = jnp.arange(spots, dtype=jnp.int32)
    earlier = order[None, :] < order[:, None]
    rank = jnp.sum(jnp.where(earlier[None], mask[:, None, :], 0.0), axis=2).astype(jnp.int32)
    first = jnp.arange(sources, dtype=jnp.int32)[:, None] * stride
    offset = jnp.where(mask > 0, first + rank * block_size, -1)
    offset = offset.reshape(row_count, cols_per_row, layer_count, row_blocks, q_blocks)
    offset = offset.transpose(1, 4, 2, 0, 3)
    offset = jnp.where(lax.axis_index("row") == 0, offset[:, :, :, ::-1], offset)
    scale = jnp.repeat(b_mask.astype(jnp.float32), block_size, axis=1)
    theirs, mine = multiply(offset.reshape(-1), scale, gathered, b_dense, block_size, all_rows)
    return mine + lax.ppermute(theirs, "row", [(0, 1), (1, 0)])


def solution(mesh):
    placed = (
        P("layer", "row", "col"),
        P("layer", "row", "col"),
        P("row", ("col", "layer")),
        P("row", ("col", "layer")),
    )
    pair = mesh.shape["row"] == 2 and mesh.shape["col"] % 2 == 0
    return jax.shard_map(
        on_pair_device if pair else on_device,
        mesh=mesh, in_specs=placed, out_specs=P("row", ("col", "layer")), check_vma=False,
    )
```

```python
import functools

import jax
import jax.numpy as jnp
from jax import lax
from jax.experimental import pallas as pl
from jax.experimental.pallas import tpu as pltpu
from jax.sharding import PartitionSpec as P

precise = lax.Precision.HIGHEST


def to_blocks(matrix, block_size):
    row_blocks = matrix.shape[0] // block_size
    col_blocks = matrix.shape[1] // block_size
    shaped = matrix.reshape(row_blocks, block_size, col_blocks, block_size).transpose(0, 2, 1, 3)
    return shaped.reshape(row_blocks * col_blocks, block_size, block_size)


def pack_blocks(blocks, is_live, capacity):
    total_places = is_live.shape[0]
    rank_of = jnp.cumsum(is_live) - 1
    slot_numbers = jnp.arange(capacity, dtype=jnp.int32)
    chosen = (is_live[None, :] > 0) & (rank_of[None, :] == slot_numbers[:, None])
    weights = chosen.astype(jnp.float32)
    packed = jnp.einsum("cg,gxy->cxy", weights, blocks, precision=precise)
    places = jnp.arange(total_places, dtype=jnp.int32)
    any_match = jnp.any(chosen, axis=1)
    position = jnp.sum(jnp.where(chosen, places[None, :], 0), axis=1)
    slot_ids = jnp.where(any_match, position, -1)
    return (packed, slot_ids)


def lookup_table(gathered, key_of, key_count):
    slot_count = gathered.shape[0]
    key_values = jnp.arange(key_count, dtype=jnp.int32)
    matches = key_of[:, None] == key_values[None, :]
    any_match = jnp.any(matches, axis=0)
    slot_numbers = jnp.arange(slot_count, dtype=jnp.int32)
    slot_index = jnp.sum(jnp.where(matches, slot_numbers[:, None], 0), axis=0)
    slot_of = jnp.where(any_match, slot_index, slot_count)
    padded = jnp.concatenate([gathered, jnp.zeros((1,) + gathered.shape[1:], jnp.float32)], axis=0)
    return (padded, slot_of)


def accumulate(running, slot_data, slot_ids, source, padded, slot_of, k_step, jwidth):
    row_blocks = running.shape[0]
    is_live = slot_ids >= 0
    clipped = jnp.maximum(slot_ids, 0)
    k_index = source * k_step + clipped // jwidth
    column = clipped % jwidth
    rows_here = jnp.arange(row_blocks, dtype=jnp.int32)
    where_rows = slot_of[k_index[:, None] * row_blocks + rows_here[None, :]]
    a_pieces = padded[where_rows]
    b_pieces = jnp.where(is_live[:, None, None], slot_data, 0.0)
    products = jnp.einsum("smxa,sab->smxb", a_pieces, b_pieces, precision=precise)
    spread = (
        (column[:, None] == jnp.arange(jwidth, dtype=jnp.int32)[None, :]) & is_live[:, None]
    ).astype(jnp.float32)
    return running + jnp.einsum("smxb,sj->mxjb", products, spread, precision=precise)


def make_folder(padded, slot_of, k_step, jwidth, shard):

    def fold_piece(running, portion, offset):
        slot_data, slot_ids = portion
        sources = slot_data.shape[0] // shard
        slot_groups = slot_data.reshape((sources, shard) + slot_data.shape[1:])
        id_groups = slot_ids.reshape(sources, shard)
        source_rows = jnp.arange(sources, dtype=jnp.int32)

        def add_source(carry, inputs):
            group_slots, group_ids, source = inputs
            return (
                accumulate(carry, group_slots, group_ids, source, padded, slot_of, k_step, jwidth),
                None,
            )

        result, unused = lax.scan(add_source, running, (slot_groups, id_groups, source_rows))
        return result

    return fold_piece


def on_device(a_cyclic, a_mask, b_dense, b_mask):
    block_size = a_cyclic.shape[1] // a_mask.shape[1]
    layer_count = lax.axis_size("layer")
    row_count = lax.axis_size("row")
    row_blocks = a_mask.shape[1]
    q_blocks = a_mask.shape[2]
    k_run = b_mask.shape[0]
    j_run = b_mask.shape[1]
    per_layer = k_run // layer_count
    a_capacity = max(2, row_blocks * q_blocks * 3 // 8)
    b_capacity = max(2, per_layer * j_run * 3 // 8)
    a_blocks = to_blocks(a_cyclic[0], block_size)
    a_slots, a_ids = pack_blocks(a_blocks, a_mask[0].reshape(-1), a_capacity)
    b_blocks = to_blocks(b_dense, block_size)
    gathered, gathered_ids = (
        lax.all_gather(a_slots, ("col", "layer"), axis=0, tiled=True),
        lax.all_gather(a_ids, ("col", "layer"), axis=0, tiled=True),
    )
    from_device = jnp.arange(gathered.shape[0], dtype=jnp.int32) // a_capacity
    from_col = from_device // layer_count
    from_layer = from_device % layer_count
    clipped = jnp.maximum(gathered_ids, 0)
    k_index = (from_col * q_blocks + clipped % q_blocks) * layer_count + from_layer
    key_of = jnp.where(gathered_ids >= 0, k_index * row_blocks + clipped // q_blocks, -1)
    padded, slot_of = lookup_table(gathered, key_of, k_run * row_count * row_blocks)
    b_slots, b_ids = pack_blocks(b_blocks, b_mask.reshape(-1), layer_count * b_capacity)
    zero_sum = jnp.zeros((row_blocks, block_size, j_run, block_size), jnp.float32)
    folder = make_folder(padded, slot_of, k_run, j_run, layer_count * b_capacity)
    running = folder(
        zero_sum,
        (
            lax.all_gather(b_slots, "row", axis=0, tiled=True),
            lax.all_gather(b_ids, "row", axis=0, tiled=True),
        ),
        jnp.int32(0),
    )
    return running.reshape(row_blocks * block_size, j_run * block_size)


CHUNK = 2
PIECES = 2
DEPTH = 4
MASK_ROWS = 8


def pack_kernel(block_size, capacity, places, mask_ref, a_ref, out_ref, sems):
    copies = []
    for slot in range(capacity):
        row = pl.multiple_of(places[0, slot] * block_size, block_size)
        column = pl.multiple_of(places[1, slot] * block_size, block_size)
        copies.append(
            pltpu.make_async_copy(
                a_ref.at[pl.ds(row, block_size), pl.ds(column, block_size)],
                out_ref.at[pl.ds(slot * block_size, block_size), :],
                sems.at[slot],
            )
        )
    for copy in copies:
        copy.start()
    out_ref[pl.ds(capacity * block_size, MASK_ROWS), :] = mask_ref[...]
    for copy in copies:
        copy.wait()


def pack_a(a_local, mask, block_size, capacity):
    row_blocks, q_blocks = mask.shape
    flat = mask.reshape(-1)
    spots = row_blocks * q_blocks
    order = jnp.arange(spots, dtype=jnp.int32)
    before = jnp.sum(jnp.where(order[None, :] < order[:, None], flat[None, :], 0), axis=1)
    slots = jnp.arange(capacity, dtype=jnp.int32)
    chosen = (flat[None, :] > 0) & (before[None, :] == slots[:, None])
    position = jnp.sum(jnp.where(chosen, order[None, :], 0), axis=1)
    places = jnp.stack([position // q_blocks, position % q_blocks])
    mask_rows = jnp.zeros((MASK_ROWS, block_size), jnp.float32)
    mask_rows = mask_rows.at[0, :spots].set(flat.astype(jnp.float32))
    return pl.pallas_call(
        functools.partial(pack_kernel, block_size, capacity),
        out_shape=jax.ShapeDtypeStruct((capacity * block_size + MASK_ROWS, block_size), jnp.float32),
        in_specs=[
            pl.BlockSpec(memory_space=pltpu.SMEM),
            pl.BlockSpec(memory_space=pltpu.VMEM),
            pl.BlockSpec(memory_space=pl.ANY),
        ],
        out_specs=pl.BlockSpec(memory_space=pltpu.VMEM),
        scratch_shapes=[pltpu.SemaphoreType.DMA((capacity,))],
    )(places, mask_rows, a_local)


def split(value):
    high = value.astype(jnp.bfloat16)
    low = (value - high.astype(jnp.float32)).astype(jnp.bfloat16)
    return high, low


def product_kernel(
    block_size, row_blocks, first_column, table, base_ref, scale_ref, a_ref, b_ref, total,
    blocks, tile, high_ref, low_ref, offset_of, row_of, sems, a_sem
):
    k_run, width = scale_ref.shape

    def fetch(k):
        slot = lax.rem(k, DEPTH)
        row = pl.multiple_of(k * block_size, block_size)
        return pltpu.make_async_copy(
            b_ref.at[pl.ds(row, block_size), pl.ds(first_column, width)],
            tile.at[slot],
            sems.at[slot],
        )

    start_row = pl.multiple_of(base_ref[0], MASK_ROWS)
    whole = pltpu.make_async_copy(
        a_ref.at[pl.ds(start_row, blocks.shape[0]), :], blocks, a_sem
    )
    for k in range(DEPTH - 1):
        fetch(k).start()
    whole.start()
    total[...] = jnp.zeros_like(total)
    whole.wait()

    @pl.loop(0, k_run)
    def step(k):
        @pl.when(k + DEPTH - 1 < k_run)
        def ahead():
            fetch(k + DEPTH - 1).start()

        count = jnp.int32(0)
        for m in range(row_blocks):
            offset = table[k * row_blocks + m]
            offset_of[count] = offset
            row_of[count] = m
            count = count + (offset >= 0).astype(jnp.int32)
        fetch(k).wait()

        @pl.when(count > 0)
        def used():
            slot = lax.rem(k, DEPTH)
            high, low = split(tile[slot] * scale_ref[pl.ds(k, 1), :])
            high_ref[pl.ds(0, block_size), :] = high
            high_ref[pl.ds(block_size, block_size), :] = high
            low_ref[pl.ds(0, block_size), :] = low
            low_ref[pl.ds(block_size, block_size), :] = low

            def left_of(places):
                pieces = []
                for place in places:
                    start = pl.multiple_of(offset_of[place], MASK_ROWS)
                    a_high, a_low = split(blocks[pl.ds(start, block_size), :])
                    pieces.append(jnp.concatenate([a_high, a_low], axis=1))
                return jnp.concatenate(pieces, axis=0)

            def add(places):
                left = left_of(places)
                part = jnp.dot(left, high_ref[...], preferred_element_type=jnp.float32)
                part = part + jnp.dot(left, low_ref[...], preferred_element_type=jnp.float32)
                for i, place in enumerate(places):
                    row = pl.multiple_of(row_of[place] * block_size, block_size)
                    total[pl.ds(row, block_size), :] += part[i * block_size:(i + 1) * block_size]

            @pl.loop(0, count // CHUNK)
            def chunk(c):
                add([c * CHUNK + i for i in range(CHUNK)])

            @pl.when(count % CHUNK == 1)
            def last():
                add([count - 1])


def multiply(table, base, scale, gathered, b_local, block_size, row_blocks, first_column, width):
    k_run = b_local.shape[0] // block_size
    vmem = pl.BlockSpec(memory_space=pltpu.VMEM)
    smem = pl.BlockSpec(memory_space=pltpu.SMEM)
    hbm = pl.BlockSpec(memory_space=pl.ANY)
    part = scale[:, first_column:first_column + width]
    return pl.pallas_call(
        functools.partial(product_kernel, block_size, row_blocks, first_column),
        out_shape=jax.ShapeDtypeStruct((row_blocks * block_size, width), jnp.float32),
        in_specs=[smem, smem, vmem, hbm, hbm],
        out_specs=vmem,
        scratch_shapes=[
            pltpu.VMEM((gathered.shape[0] // 2, block_size), jnp.float32),
            pltpu.VMEM((DEPTH, block_size, width), jnp.float32),
            pltpu.VMEM((2 * block_size, width), jnp.bfloat16),
            pltpu.VMEM((2 * block_size, width), jnp.bfloat16),
            pltpu.SMEM((row_blocks + CHUNK,), jnp.int32),
            pltpu.SMEM((row_blocks + CHUNK,), jnp.int32),
            pltpu.SemaphoreType.DMA((DEPTH,)),
            pltpu.SemaphoreType.DMA,
        ],
        compiler_params=pltpu.CompilerParams(vmem_limit_bytes=56 * 1024 * 1024),
        cost_estimate=pl.CostEstimate(
            flops=4 * k_run * row_blocks * block_size * block_size * width,
            bytes_accessed=4 * k_run * block_size * width,
            transcendentals=0,
        ),
    )(table, base, part, gathered, b_local)


def gather_a(payload, cols_per_row):
    row_count, col_count = lax.axis_size("row"), lax.axis_size("col")
    pairs = []
    for row in range(row_count):
        for col in range(col_count):
            target = (col // cols_per_row) * col_count + row * cols_per_row + col % cols_per_row
            pairs.append((row * col_count + col, target))
    moved = lax.ppermute(payload, ("row", "col"), pairs)
    return lax.all_gather(moved, ("col", "layer"), axis=0, tiled=True)


def on_pair_device(a_cyclic, a_mask, b_dense, b_mask):
    row_blocks, q_blocks = a_mask.shape[1:]
    block_size = a_cyclic.shape[1] // row_blocks
    layer_count, row_count = lax.axis_size("layer"), lax.axis_size("row")
    cols_per_row = lax.axis_size("col") // row_count
    capacity = max(2, row_blocks * q_blocks * 3 // 8)
    payload = pack_a(a_cyclic[0], a_mask[0], block_size, capacity)
    gathered = gather_a(payload, cols_per_row)
    spots = row_blocks * q_blocks
    stride = payload.shape[0]
    sources = gathered.shape[0] // stride
    mask = gathered.reshape(sources, stride, block_size)[:, capacity * block_size, :spots]
    order = jnp.arange(spots, dtype=jnp.int32)
    earlier = order[None, :] < order[:, None]
    rank = jnp.sum(jnp.where(earlier[None], mask[:, None, :], 0.0), axis=2).astype(jnp.int32)
    per_row = sources // row_count
    first = (jnp.arange(sources, dtype=jnp.int32)[:, None] % per_row) * stride
    offset = jnp.where(mask > 0, first + rank * block_size, -1)
    offset = offset.reshape(row_count, cols_per_row, layer_count, row_blocks, q_blocks)
    offset = offset.transpose(0, 1, 4, 2, 3).reshape(row_count, -1)
    scale = jnp.repeat(b_mask.astype(jnp.float32), block_size, axis=1)
    width = b_dense.shape[1]
    me = lax.axis_index("row")

    def rows_of(row, first_column, columns):
        base = (row * per_row * stride).astype(jnp.int32).reshape(1)
        table = jnp.where(row == 0, offset[0], offset[1])
        return multiply(
            table, base, scale, gathered, b_dense, block_size, row_blocks, first_column, columns
        )

    piece = width // PIECES
    received = []
    for i in range(PIECES):
        theirs = rows_of(1 - me, i * piece, piece)
        received.append(lax.ppermute(theirs, "row", [(0, 1), (1, 0)]))
    mine = rows_of(me, 0, width)
    return mine + jnp.concatenate(received, axis=1)


def solution(mesh):
    placed = (
        P("layer", "row", "col"),
        P("layer", "row", "col"),
        P("row", ("col", "layer")),
        P("row", ("col", "layer")),
    )
    pair = mesh.shape["row"] == 2 and mesh.shape["col"] % 2 == 0
    return jax.shard_map(
        on_pair_device if pair else on_device,
        mesh=mesh, in_specs=placed, out_specs=P("row", ("col", "layer")), check_vma=False,
    )
```
